32 devices in a mesh: shot: 8 (over z, y), rcv: 4 (over x, core).
Axes of the slice: x: 2, y: 2, z: 4, core: 2. Of those that a mesh axis runs over, the one named last changes fastest.
Arguments:
- shot_data: bfloat16 [256, 1024, 256], P('shot', 'rcv'), may hold values from -0.375 to 0.375
- code: int32 [32, 256], P(None, 'shot'), may hold values from -1 to 1, as said below
- observed: bfloat16 [32, 1024, 256], P('shot', 'rcv'), may hold values from -6 to 6
- block_of: int32 [1024, 1], replicated, may hold values from 0 to 3; in each aligned block of 256 rows (0 to 255, 256 to 511, ...) at most 64 rows name the same one
- stencil_index: int32 [1024, 4], replicated, may hold values from 0 to 255
- stencil_weight: float32 [1024, 4], replicated, may hold values from -0.5 to 1
Outputs:
- adjoint_source: float32 [32, 1024, 256], P('shot', 'rcv')
The draws below stay inside these ranges and needn't reach their ends.
Inputs may be any that keep to these rules, and one draw needn't show every extreme that they name: `code`: every entry is -1 or 1. `block_of`: among the receivers of one index of rcv (aligned blocks of 256 rows) at most 64 map to one model block.
All inputs are finite; a program needn't handle non-finite values.
Results may differ from the reference program's by a relative error of at most 0.0038.
Values may be sent and summed in bfloat16 or wider, within the bound.
No kernel may reach another device: no remote copies, remote signals or barrier semaphores. Data moves between devices by JAX's collectives and lax.ppermute only.
A program may use at most 64 MiB of HBM per device.

```python
import math
import jax
import jax.numpy as jnp
import numpy as np
from jax import lax

SUPERS = 32
RCV_DEV = 256
SAMPLES = 256
GRID = 256
STENCIL = 4
CAP = 64
SHOTS = 256
RECEIVERS = 1024
BLOCKS = 4


def draw_code(key, part):
    return (2 * jax.random.randint(key, (SUPERS, SHOTS), 0, 2) - 1).astype(jnp.int32)


def plant(array, own_key, least, largest):
    dims = array.shape
    index_at = [jax.random.randint(jax.random.fold_in(own_key, axis), (), 0, dims[axis]) for axis in range(len(dims))]
    array = array.at[tuple(index_at)].set(least)
    longest = dims.index(max(dims))
    index_at[longest] = (index_at[longest] + 1) % dims[longest]
    return array.at[tuple(index_at)].set(largest)


def level_of(rng, shape, shards, smallest, high):
    loudness = 1.0
    for axis_at, shards_of in shards:
        draws = jax.random.uniform(jax.random.fold_in(jax.random.fold_in(rng, 6), axis_at), (shards_of,), jnp.float32, smallest / len(shards), high / len(shards))
        loudness = loudness * jnp.repeat(jnp.exp(draws), shape[axis_at] // shards_of).reshape((-1,) + (1,) * (len(shape) - 1 - axis_at))
    return loudness


def deal_out(rng, own, number, rows, number_of, top, bound, skew):
    order = jax.random.permutation(rng, number_of)
    packed, common = shares(number_of, rows * top, bound, skew, True), shares(number_of, rows * top, bound, skew, False)
    places = jnp.arange(number_of)

    def named(lengths, rotation):
        used = int((lengths > 0).sum())
        fixed = max(1, used // 4)
        shifted = fixed + (places - fixed + rotation * (used - fixed)) % max(1, number_of - fixed)
        return jnp.zeros((number_of,), jnp.int32).at[order[jnp.where(places < fixed, places, shifted)]].set(jnp.asarray(lengths, jnp.int32))

    lengths = jnp.where(number % 4 == 0, named(packed, number // 4), named(common, number - number // 4 - 1))
    mixed = jax.random.permutation(jax.random.fold_in(own, 3), number_of)
    giver, taker = mixed[0:number_of // 2 * 2:2], mixed[1:number_of // 2 * 2:2]
    room = jnp.minimum(lengths[giver] - 1, bound - lengths[taker]) // 2
    room = jnp.where((giver == order[0]) | (taker == order[0]) | (lengths[taker] == 0), 0, jnp.maximum(room, 0))
    shifted = jax.random.randint(jax.random.fold_in(own, 4), (number_of // 2,), 0, 1 << 20) % (room + 1)
    lengths = lengths.at[giver].add(-shifted).at[taker].add(shifted)
    items = jnp.searchsorted(jnp.cumsum(lengths), jnp.arange(rows * top), side="right").astype(jnp.int32)
    listing = items.reshape(top, rows).T
    listing = listing[jax.random.permutation(jax.random.fold_in(own, 1), rows)]
    rotation = jax.random.randint(jax.random.fold_in(own, 2), (rows, 1), 0, top)
    return jnp.take_along_axis(listing, (jnp.arange(top)[None, :] + rotation) % top, axis=1)


def shares(number_of, total, bound, skew, full):
    weights = [(1 << 20) // math.isqrt(rank ** skew) + 1 for rank in range(1, number_of + 1)]
    largest = bound if full else min(bound, max(-(-total // number_of), total * weights[0] // sum(weights)))
    least = 1 if total - largest >= number_of - 1 else 0
    given, spare = [largest] + [least] * (number_of - 1), total - largest - least * (number_of - 1)
    while spare > 0:
        candidates = [i for i in range(1, number_of) if given[i] < largest] or [i for i in range(1, number_of) if given[i] < bound]
        mass, remaining = sum([weights[i] for i in candidates]), spare
        for i in candidates:
            addition = min(bound - given[i], max(1, remaining * weights[i] // mass), spare)
            given[i] = given[i] + addition
            spare = spare - addition
    return np.array(given)


def noise(key, extent, scale, reach, cuts=(), kind=jnp.bfloat16):
    values = jax.random.normal(key, extent, jnp.float32) * scale
    if len(cuts) > 0:
        values = level_of(key, extent, cuts, -0.22, 0.18) * values
    return jnp.clip(values, min=-reach, max=reach).astype(kind)


def setup_inputs(seed: int = 0) -> dict:
    seeds = jax.random.split(jax.random.key(seed), 7)
    shot_data = noise(seeds[0], (SHOTS, RECEIVERS, SAMPLES), SHOTS ** -0.5, 0.375, ((0, 8), (1, 4)))
    code = draw_code(jax.random.fold_in(seeds[6], 71), 0)
    observed = noise(seeds[2], (SUPERS, RECEIVERS, SAMPLES), 1.0, 6.0, ((0, 8), (1, 4)))
    block_of_keys = jax.random.split(jax.random.fold_in(seeds[3], 1), RECEIVERS // RCV_DEV)
    block_of_turns = jax.random.permutation(jax.random.fold_in(seeds[3], 3), RECEIVERS // RCV_DEV)
    block_of = jax.vmap(lambda own, number: deal_out(jax.random.fold_in(seeds[3], 2), own, number, RCV_DEV, BLOCKS, 1, CAP, 2))(block_of_keys, block_of_turns).reshape((RECEIVERS, 1))
    stencil_index = plant(jax.random.randint(seeds[4], (RECEIVERS, STENCIL), 0, GRID), jax.random.fold_in(seeds[4], 1), 0, GRID - 1).astype(jnp.int32)
    stencil_weight = jnp.clip(jax.random.uniform(seeds[5], (RECEIVERS, STENCIL), jnp.float32, -0.5, 1.0), -0.5, 1.0)
    return {"shot_data": shot_data, "code": code, "observed": observed, "block_of": block_of, "stencil_index": stencil_index, "stencil_weight": stencil_weight}


def spread_weights(stencil_index, stencil_weight):
    receivers = stencil_index.shape[0]
    points = jnp.arange(GRID, dtype=jnp.int32)[:, None]
    spread = jnp.zeros((GRID, receivers), jnp.float32)
    for which in range(STENCIL):
        spread = spread + jnp.where(points == stencil_index[:, which][None, :], stencil_weight[:, which][None, :], 0.0)
    return spread


def reference(shot_data, code, observed, block_of, stencil_index, stencil_weight):
    shots, receivers, samples = shot_data.shape
    flat_rows = shot_data.reshape(shots, receivers * samples)
    supershot = jnp.dot(code.astype(jnp.bfloat16), flat_rows, preferred_element_type=jnp.float32)
    supershot = supershot.reshape(SUPERS, receivers, samples)
    residual = (supershot - observed.astype(jnp.float32)).astype(jnp.bfloat16)
    spread = spread_weights(stencil_index, stencil_weight)
    block_ids = jnp.arange(BLOCKS, dtype=jnp.int32)[:, None, None]
    injection = jnp.where(block_ids == block_of[:, 0][None, None, :], spread[None], 0.0)
    injection = injection.reshape(BLOCKS * GRID, receivers).astype(jnp.bfloat16)
    return jnp.einsum("cr,krt->kct", injection.astype(jnp.float32), residual.astype(jnp.float32), precision=lax.Precision.HIGHEST)
```

```python
import jax
import jax.numpy as jnp
from jax import lax
from jax.sharding import PartitionSpec as P

GRID = 256
STENCIL = 4
CAP = 64
ROW_TILE = 16


def link_masks(size):
    masks, bit = [], size.bit_length() - 2
    while bit >= 0:
        if bit >= 1:
            masks += [1 << (bit - 1), (1 << bit) | (1 << (bit - 1))]
            bit -= 2
        else:
            masks.append(1)
            bit -= 1
    return masks


def spread_weights(stencil_index, stencil_weight):
    receivers = stencil_index.shape[0]
    points = jnp.arange(GRID, dtype=jnp.int32)[:, None]
    spread = jnp.zeros((GRID, receivers), jnp.float32)
    for which in range(STENCIL):
        spread = spread + jnp.where(
            points == stencil_index[:, which][None, :], stencil_weight[:, which][None, :], 0.0
        )
    return spread


def swap(value, axis, size, mask):
    return lax.ppermute(value, axis, [(i, i ^ mask) for i in range(size)])


def scatter_sum(shot_data, code, owned):
    n_shot = lax.axis_size("shot")
    shot_dev, rcv_dev, samples = shot_data.shape
    me = lax.axis_index("shot")
    masks = link_masks(n_shot)
    groups = len(masks)
    tiles = rcv_dev // ROW_TILE
    bounds = [tiles * g // groups * ROW_TILE for g in range(groups)] + [rcv_dev]
    rows = code.astype(jnp.bfloat16).reshape(n_shot, owned * shot_dev)
    everyone = jnp.arange(n_shot, dtype=jnp.int32)
    held = []
    for g in range(groups):
        order = masks[g:] + masks[:g]
        relative = [0]
        for mask in reversed(order):
            relative = relative + [e ^ mask for e in relative]
        wanted = me ^ jnp.array(relative, jnp.int32)
        pick = (wanted[:, None] == everyone[None, :]).astype(jnp.bfloat16)
        signs = jnp.dot(pick, rows, preferred_element_type=jnp.float32).astype(jnp.bfloat16)
        signs = signs.reshape(n_shot, owned, shot_dev)
        part = shot_data[:, bounds[g] : bounds[g + 1], :]
        half = n_shot // 2
        send = jnp.einsum(
            "eos,srt->eort", signs[half:], part, preferred_element_type=jnp.float32
        ).astype(jnp.bfloat16)
        keep = jnp.einsum("eos,srt->eort", signs[:half], part, preferred_element_type=jnp.float32)
        held.append((order, keep, send))
    for step in range(len(masks)):
        arrived = [swap(send, "shot", n_shot, order[step]) for order, _, send in held]
        later = []
        for (order, keep, _), came in zip(held, arrived):
            total = keep + came.astype(jnp.float32)
            half = total.shape[0] // 2
            later.append((order, total[:half], total[half:].astype(jnp.bfloat16)) if half else (order, total, None))
        held = later
    return [total[0] for _, total, _ in held], bounds


def on_device(shot_data, code, observed, block_of, stencil_index, stencil_weight):
    shot_dev, rcv_dev, samples = shot_data.shape
    owned = observed.shape[0]
    sums, bounds = scatter_sum(shot_data, code, owned)
    n_blocks = lax.axis_size("rcv")
    my_block = lax.axis_index("rcv")
    block_ids = block_of[:, 0]
    spread = spread_weights(stencil_index, stencil_weight)
    own_matrix = jnp.where(block_ids[None, :] == my_block, spread, 0.0).astype(jnp.bfloat16)
    my_ids = lax.dynamic_slice_in_dim(block_ids, my_block * rcv_dev, rcv_dev, 0)
    block_range = my_block ^ jnp.arange(n_blocks, dtype=jnp.int32)
    onehot = (my_ids[:, None] == block_range[None, :]).astype(jnp.int32)
    slot_rank = jnp.sum((jnp.cumsum(onehot, axis=0) - 1) * onehot, axis=1)
    slot_range = jnp.arange(CAP, dtype=jnp.int32)
    selection = (my_ids[None, None, :] == block_range[:, None, None]) & (
        slot_rank[None, None, :] == slot_range[None, :, None]
    )
    selection = selection.reshape(n_blocks * CAP, rcv_dev).astype(jnp.bfloat16)
    residual = jnp.concatenate(
        [
            (total - observed[:, low:high, :].astype(jnp.float32)).astype(jnp.bfloat16)
            for total, low, high in zip(sums, bounds[:-1], bounds[1:])
        ],
        axis=1,
    )
    outgoing = jnp.einsum(
        "sr,krt->kst", selection, residual, preferred_element_type=jnp.float32
    ).astype(jnp.bfloat16)
    pieces = [outgoing[:, :CAP]] + [
        swap(outgoing[:, e * CAP : (e + 1) * CAP], "rcv", n_blocks, e) for e in range(1, n_blocks)
    ]
    incoming = jnp.concatenate(pieces, axis=1)
    mine_all = (block_ids.reshape(n_blocks, rcv_dev) == my_block).astype(jnp.int32)
    rank_all = jnp.cumsum(mine_all, axis=1) - 1
    pick_all = (
        (mine_all[:, :, None] == 1) & (rank_all[:, :, None] == slot_range[None, None, :])
    ).astype(jnp.float32)
    slot_matrix = jnp.einsum(
        "gdr,drc->dgc", own_matrix.astype(jnp.float32).reshape(GRID, n_blocks, rcv_dev), pick_all
    ).astype(jnp.bfloat16)
    slot_matrix = jnp.stack(
        [lax.dynamic_index_in_dim(slot_matrix, my_block ^ e, 0, keepdims=False) for e in range(n_blocks)],
        axis=1,
    )
    slot_matrix = slot_matrix.reshape(GRID, n_blocks * CAP)
    return jnp.einsum("cs,kst->kct", slot_matrix, incoming, preferred_element_type=jnp.float32)


def solution(mesh):
    placed = (P("shot", "rcv", None), P(None, "shot"), P("shot", "rcv", None), P(), P(), P())
    return jax.shard_map(
        on_device, mesh=mesh, in_specs=placed, out_specs=P("shot", "rcv", None), check_vma=False
    )
```

```python
import functools
import jax
import jax.numpy as jnp
from jax import lax
from jax.experimental import pallas as pl
from jax.experimental.pallas import tpu as pltpu
from jax.sharding import PartitionSpec as P

GRID = 256
STENCIL = 4
CAP = 64
GROUP = 8
FAR_END, FAR_MID, MATE, OWN = range(4)
LINE = 4


def spread_weights(stencil_index, stencil_weight):
    receivers = stencil_index.shape[0]
    points = jnp.arange(GRID, dtype=jnp.int32)[:, None]
    spread = jnp.zeros((GRID, receivers), jnp.float32)
    for which in range(STENCIL):
        spread = spread + jnp.where(
            points == stencil_index[:, which][None, :], stencil_weight[:, which][None, :], 0.0
        )
    return spread


def wide(value):
    return value.astype(jnp.float32)


def narrow(value):
    return value.astype(jnp.bfloat16)


def swap(value, axis, size, mask):
    return lax.ppermute(value, axis, [(i, i ^ mask) for i in range(size)])


def along_line(value, inner, moves):
    pairs = [(a * inner + i, b * inner + i) for a, b in moves for i in range(inner)]
    return lax.ppermute(value, "shot", pairs)


def partial_sums_kernel(inner, owned, outputs, data_ref, code_ref, *refs):
    out_refs, mix_ref = refs[:-1], refs[-1]
    shot_dev, rows, samples = data_ref.shape
    me = lax.axis_index("shot")
    place = lax.div(me, inner)
    column = lax.rem(me, inner)
    low = place < LINE // 2
    targets = {
        FAR_END: jnp.where(low, LINE - 1, 0),
        FAR_MID: jnp.where(low, LINE // 2, LINE // 2 - 1),
        MATE: place ^ 1,
        OWN: place,
    }

    @pl.when(pl.program_id(0) == 0)
    def _():
        picked = []
        for wanted, _ in outputs:
            for label, other, row in wanted:
                at = (targets[label] * inner + (column ^ other)) * owned + row
                picked.append(jnp.broadcast_to(code_ref[pl.ds(at, 1), :], (GROUP, shot_dev)))
        signs = narrow(jnp.concatenate(picked, axis=0).astype(jnp.float32))
        width = shot_dev * GROUP
        shot = lax.broadcasted_iota(jnp.int32, (shot_dev, width), 0)
        lane = lax.broadcasted_iota(jnp.int32, (shot_dev, width), 1)
        spread = narrow(wide(shot == lane // GROUP))
        mixed = jnp.dot(signs, spread, preferred_element_type=jnp.float32)
        sub = lax.broadcasted_iota(jnp.int32, mixed.shape, 0)
        lane = lax.broadcasted_iota(jnp.int32, mixed.shape, 1)
        mix_ref[...] = narrow(jnp.where(sub % GROUP == lane % GROUP, mixed, 0.0))

    mix = mix_ref[...]
    for group in range(rows // GROUP):
        part = data_ref[:, group * GROUP : (group + 1) * GROUP, :].reshape(shot_dev * GROUP, samples)
        product = jnp.dot(mix, part, preferred_element_type=jnp.float32)
        at = 0
        for (wanted, _), ref in zip(outputs, out_refs):
            for entry in range(len(wanted)):
                piece = product[at * GROUP : (at + 1) * GROUP]
                ref[entry, group * GROUP : (group + 1) * GROUP, :] = piece.astype(ref.dtype)
                at += 1


def partial_sums(shot_data, code, inner, owned, outputs):
    shot_dev, rcv_dev, samples = shot_data.shape
    supers = code.shape[0]
    block = rcv_dev // 4
    return pl.pallas_call(
        functools.partial(partial_sums_kernel, inner, owned, outputs),
        grid=(rcv_dev // block,),
        in_specs=[
            pl.BlockSpec((shot_dev, block, samples), lambda i: (0, i, 0)),
            pl.BlockSpec(code.shape, lambda i: (0, 0)),
        ],
        out_specs=[pl.BlockSpec((len(w), block, samples), lambda i: (0, i, 0)) for w, _ in outputs],
        out_shape=[jax.ShapeDtypeStruct((len(w), rcv_dev, samples), t) for w, t in outputs],
        scratch_shapes=[pltpu.VMEM((supers * GROUP, shot_dev * GROUP), jnp.bfloat16)],
        cost_estimate=pl.CostEstimate(
            flops=2 * supers * shot_dev * rcv_dev * samples * GROUP, bytes_accessed=2 * shot_data.size, transcendentals=0
        ),
    )(shot_data, code)


def scatter_sum_line(shot_data, code, owned):
    n_shot = lax.axis_size("shot")
    inner = n_shot // LINE
    half = owned // 2
    rows = [range(half), range(half, owned)]
    first, last = 0, LINE - 1
    mid, next_mid = LINE // 2 - 1, LINE // 2
    names, outputs = [], []

    def need(name, blocks, part, dtype):
        names.append(name)
        outputs.append(([(label, other, row) for label, other in blocks for row in rows[part]], dtype))

    need("mate0", [(MATE, 0), (MATE, 1)], 0, jnp.bfloat16)
    for part in (0, 1):
        for label in (FAR_END, FAR_MID):
            need(("send", label, part), [(label, 1)], part, jnp.bfloat16)
            need(("keep", label, part), [(label, 0)], part, jnp.float32)
    need(("send", MATE, 1), [(MATE, 1)], 1, jnp.bfloat16)
    need(("keep", MATE, 1), [(MATE, 0)], 1, jnp.float32)
    need(("keep", OWN, 0), [(OWN, 0)], 0, jnp.float32)
    need(("other", OWN, 0), [(OWN, 1)], 0, jnp.float32)
    need(("keep", OWN, 1), [(OWN, 0)], 1, jnp.float32)
    need(("send", OWN, 1), [(OWN, 1)], 1, jnp.bfloat16)
    have = dict(zip(names, partial_sums(shot_data, code, inner, owned, outputs)))

    mates = [(first, mid), (mid, first), (last, next_mid), (next_mid, last)]
    inward = [(first, mid), (last, next_mid)]
    to_end = [(mid, last), (next_mid, first)]
    to_mid = [(mid, next_mid), (next_mid, mid)]

    def beside(value):
        return wide(swap(value, "shot", n_shot, 1))

    from_mate0 = along_line(have["mate0"], inner, mates)
    far = {}
    for part in (0, 1):
        for label, forward in ((FAR_END, to_end), (FAR_MID, to_mid)):
            both = have["keep", label, part] + beside(have["send", label, part])
            came = along_line(narrow(both), inner, inward)
            far[label, part] = along_line(narrow(both + wide(came)), inner, forward)
    both = have["keep", MATE, 1] + beside(have["send", MATE, 1])
    from_mate1 = along_line(narrow(both), inner, mates)
    own0 = have["keep", OWN, 0] + wide(from_mate0[:half])
    own0 = own0 + beside(narrow(have["other", OWN, 0] + wide(from_mate0[half:])))
    own1 = have["keep", OWN, 1] + wide(from_mate1) + beside(have["send", OWN, 1])
    return [
        own + wide(far[FAR_END, part]) + wide(far[FAR_MID, part]) for part, own in enumerate((own0, own1))
    ]


def scatter_sum_any(shot_data, code, owned):
    n_shot = lax.axis_size("shot")
    shot_dev, rcv_dev, samples = shot_data.shape
    me = lax.axis_index("shot")
    relative = [0]
    mask = 1
    while mask < n_shot:
        relative = relative + [e ^ mask for e in relative]
        mask *= 2
    wanted = me ^ jnp.array(relative, jnp.int32)
    signs = narrow(code).reshape(n_shot, owned, shot_dev)[wanted]
    total = jnp.einsum("eos,srt->eort", signs, shot_data, preferred_element_type=jnp.float32)
    while total.shape[0] > 1:
        count = total.shape[0] // 2
        total = total[:count] + wide(swap(narrow(total[count:]), "shot", n_shot, count))
    half = max(owned // 2, 1)
    return [total[0, low : low + half] for low in range(0, owned, half)]


def on_device(shot_data, code, observed, block_of, stencil_index, stencil_weight):
    shot_dev, rcv_dev, samples = shot_data.shape
    owned = observed.shape[0]
    if lax.axis_size("shot") == 2 * LINE and owned % 2 == 0:
        sums = scatter_sum_line(shot_data, code, owned)
    else:
        sums = scatter_sum_any(shot_data, code, owned)
    n_blocks = lax.axis_size("rcv")
    my_block = lax.axis_index("rcv")
    block_ids = block_of[:, 0]
    spread = spread_weights(stencil_index, stencil_weight)
    own_matrix = jnp.where(block_ids[None, :] == my_block, spread, 0.0).astype(jnp.bfloat16)
    my_ids = lax.dynamic_slice_in_dim(block_ids, my_block * rcv_dev, rcv_dev, 0)
    block_range = my_block ^ jnp.arange(n_blocks, dtype=jnp.int32)
    onehot = (my_ids[:, None] == block_range[None, :]).astype(jnp.int32)
    slot_rank = jnp.sum((jnp.cumsum(onehot, axis=0) - 1) * onehot, axis=1)
    slot_range = jnp.arange(CAP, dtype=jnp.int32)
    selection = (my_ids[None, None, :] == block_range[:, None, None]) & (
        slot_rank[None, None, :] == slot_range[None, :, None]
    )
    selection = selection.reshape(n_blocks * CAP, rcv_dev).astype(jnp.bfloat16)
    mine_all = (block_ids.reshape(n_blocks, rcv_dev) == my_block).astype(jnp.int32)
    rank_all = jnp.cumsum(mine_all, axis=1) - 1
    pick_all = (
        (mine_all[:, :, None] == 1) & (rank_all[:, :, None] == slot_range[None, None, :])
    ).astype(jnp.float32)
    slot_matrix = jnp.einsum(
        "gdr,drc->dgc", own_matrix.astype(jnp.float32).reshape(GRID, n_blocks, rcv_dev), pick_all
    ).astype(jnp.bfloat16)
    slot_matrix = jnp.stack(
        [lax.dynamic_index_in_dim(slot_matrix, my_block ^ e, 0, keepdims=False) for e in range(n_blocks)],
        axis=1,
    )
    slot_matrix = slot_matrix.reshape(GRID, n_blocks * CAP)
    results, at = [], 0
    for total in sums:
        residual = narrow(total - wide(observed[at : at + total.shape[0]]))
        at += total.shape[0]
        outgoing = narrow(jnp.einsum("sr,krt->kst", selection, residual, preferred_element_type=jnp.float32))
        pieces = [outgoing[:, :CAP]] + [
            swap(outgoing[:, e * CAP : (e + 1) * CAP], "rcv", n_blocks, e) for e in range(1, n_blocks)
        ]
        incoming = jnp.concatenate(pieces, axis=1)
        results.append(jnp.einsum("cs,kst->kct", slot_matrix, incoming, preferred_element_type=jnp.float32))
    return jnp.concatenate(results, axis=0)


def solution(mesh):
    placed = (P("shot", "rcv", None), P(None, "shot"), P("shot", "rcv", None), P(), P(), P())
    return jax.shard_map(
        on_device, mesh=mesh, in_specs=placed, out_specs=P("shot", "rcv", None), check_vma=False
    )
```

```python
import functools
import jax
import jax.numpy as jnp
from jax import lax
from jax.experimental import pallas as pl
from jax.experimental.pallas import tpu as pltpu
from jax.sharding import PartitionSpec as P

GRID = 256
STENCIL = 4
CAP = 64
GROUP = 8
FAR_END, FAR_MID, MATE, OWN = range(4)
LINE = 4


def spread_weights(stencil_index, stencil_weight):
    receivers = stencil_index.shape[0]
    points = jnp.arange(GRID, dtype=jnp.int32)[:, None]
    spread = jnp.zeros((GRID, receivers), jnp.float32)
    for which in range(STENCIL):
        spread = spread + jnp.where(
            points == stencil_index[:, which][None, :], stencil_weight[:, which][None, :], 0.0
        )
    return spread


def wide(value):
    return value.astype(jnp.float32)


def narrow(value):
    return value.astype(jnp.bfloat16)


def after(value, *earlier):
    return lax.optimization_barrier((value, *earlier))[0]


def swap(value, axis, size, mask):
    return lax.ppermute(value, axis, [(i, i ^ mask) for i in range(size)])


def along_line(value, inner, moves):
    pairs = [(a * inner + i, b * inner + i) for a, b in moves for i in range(inner)]
    return lax.ppermute(value, "shot", pairs)


def partial_sums_kernel(inner, owned, outputs, chunks, data_ref, code_ref, *refs):
    count = len(outputs)
    out_refs, staged = refs[:count], refs[count : 2 * count]
    data, signs_ref, code_sem, data_sem, out_sem = refs[2 * count :]
    shot_dev, rows, samples = data.shape
    block = rows // chunks
    code_copy = pltpu.make_async_copy(code_ref, signs_ref, code_sem)
    code_copy.start()
    copies = []
    for chunk in range(chunks):
        at = pl.ds(chunk * block, block)
        copies.append(pltpu.make_async_copy(data_ref.at[:, at, :], data.at[:, at, :], data_sem.at[chunk]))
        copies[-1].start()
    me = lax.axis_index("shot")
    place = lax.div(me, inner)
    column = lax.rem(me, inner)
    low = place < LINE // 2
    targets = {
        FAR_END: jnp.where(low, LINE - 1, 0),
        FAR_MID: jnp.where(low, LINE // 2, LINE // 2 - 1),
        MATE: place ^ 1,
        OWN: place,
    }
    width = shot_dev * GROUP
    shot = lax.broadcasted_iota(jnp.int32, (shot_dev, width), 0)
    lane = lax.broadcasted_iota(jnp.int32, (shot_dev, width), 1)
    spread = narrow(wide(shot == lane // GROUP))
    code_copy.wait()
    picked = []
    for wanted, _ in outputs:
        for label, other, row in wanted:
            at = (targets[label] * inner + (column ^ other)) * owned + row
            picked.append(jnp.broadcast_to(signs_ref[pl.ds(at, 1), :], (GROUP, shot_dev)))
    signs = narrow(jnp.concatenate(picked, axis=0).astype(jnp.float32))
    mixed = jnp.dot(signs, spread, preferred_element_type=jnp.float32)
    sub = lax.broadcasted_iota(jnp.int32, mixed.shape, 0)
    lane = lax.broadcasted_iota(jnp.int32, mixed.shape, 1)
    mix = narrow(jnp.where(sub % GROUP == lane % GROUP, mixed, 0.0))
    leaving = []
    for chunk in range(chunks):
        copies[chunk].wait()
        for low_row in range(chunk * block, (chunk + 1) * block, GROUP):
            part = data[:, low_row : low_row + GROUP, :].reshape(width, samples)
            product = jnp.dot(mix, part, preferred_element_type=jnp.float32)
            at = 0
            for (wanted, _), ref in zip(outputs, staged):
                for entry in range(len(wanted)):
                    piece = product[at * GROUP : (at + 1) * GROUP]
                    ref[entry, low_row : low_row + GROUP, :] = piece.astype(ref.dtype)
                    at += 1
        where = pl.ds(chunk * block, block)
        for which in range(count):
            leaving.append(
                pltpu.make_async_copy(
                    staged[which].at[:, where, :], out_refs[which].at[:, where, :], out_sem.at[which, chunk]
                )
            )
            leaving[-1].start()
    for copy in leaving:
        copy.wait()


def partial_sums(shot_data, code, inner, owned, needs, name):
    names, outputs = list(needs), list(needs.values())
    shot_dev, rcv_dev, samples = shot_data.shape
    chunks = 4
    total = sum(len(w) for w, _ in outputs)
    shapes = [((len(w), rcv_dev, samples), t) for w, t in outputs]
    anywhere = pl.BlockSpec(memory_space=pl.ANY)
    results = pl.pallas_call(
        functools.partial(partial_sums_kernel, inner, owned, outputs, chunks),
        in_specs=[anywhere, anywhere],
        out_specs=[anywhere] * len(outputs),
        out_shape=[jax.ShapeDtypeStruct(s, t) for s, t in shapes],
        scratch_shapes=[pltpu.VMEM(s, t) for s, t in shapes]
        + [
            pltpu.VMEM(shot_data.shape, shot_data.dtype),
            pltpu.VMEM(code.shape, code.dtype),
            pltpu.SemaphoreType.DMA,
            pltpu.SemaphoreType.DMA((chunks,)),
            pltpu.SemaphoreType.DMA((len(outputs), chunks)),
        ],
        cost_estimate=pl.CostEstimate(
            flops=2 * total * shot_dev * rcv_dev * samples * GROUP,
            bytes_accessed=2 * shot_data.size,
            transcendentals=0,
        ),
        name=name,
    )(shot_data, code)
    return dict(zip(names, results))


def scatter_sum_line(shot_data, code, owned):
    n_shot = lax.axis_size("shot")
    inner = n_shot // LINE
    half = owned // 2
    rows = [range(half), range(half, owned)]
    first, last = 0, LINE - 1
    mid, next_mid = LINE // 2 - 1, LINE // 2
    names, outputs = [], []

    def need(name, blocks, part, dtype):
        names.append(name)
        outputs.append(([(label, other, row) for label, other in blocks for row in rows[part]], dtype))

    need("mate0", [(MATE, 0), (MATE, 1)], 0, jnp.bfloat16)
    for part in (0, 1):
        for label in (FAR_END, FAR_MID):
            need(("send", label, part), [(label, 1)], part, jnp.bfloat16)
            need(("keep", label, part), [(label, 0)], part, jnp.float32)
    need(("send", MATE, 1), [(MATE, 1)], 1, jnp.bfloat16)
    need(("keep", MATE, 1), [(MATE, 0)], 1, jnp.float32)
    need(("keep", OWN, 0), [(OWN, 0)], 0, jnp.float32)
    need(("other", OWN, 0), [(OWN, 1)], 0, jnp.float32)
    need(("keep", OWN, 1), [(OWN, 0)], 1, jnp.float32)
    need(("send", OWN, 1), [(OWN, 1)], 1, jnp.bfloat16)
    have = partial_sums(shot_data, code, inner, owned, dict(zip(names, outputs)), "partial_sums")

    mates = [(first, mid), (mid, first), (last, next_mid), (next_mid, last)]
    inward = [(first, mid), (last, next_mid)]
    to_end = [(mid, last), (next_mid, first)]
    to_mid = [(mid, next_mid), (next_mid, mid)]

    def beside(value):
        return swap(value, "shot", n_shot, 1)

    y = {}
    from_mate0 = along_line(have["mate0"], inner, mates)
    y[FAR_END, 0] = beside(have["send", FAR_END, 0])
    y[FAR_MID, 0] = beside(have["send", FAR_MID, 0])
    y[FAR_END, 1] = beside(have["send", FAR_END, 1])
    y[FAR_MID, 1] = beside(have["send", FAR_MID, 1])
    y[MATE, 1] = beside(have["send", MATE, 1])
    y[OWN, 1] = beside(have["send", OWN, 1])
    both, came, far = {}, {}, {}
    token = have["mate0"]

    def inward_step(label, part):
        nonlocal token
        both[label, part] = after(have["keep", label, part], token) + wide(y[label, part])
        token = narrow(both[label, part])
        came[label, part] = along_line(token, inner, inward)

    def forward_step(label, part):
        nonlocal token
        forward = to_end if label == FAR_END else to_mid
        token = narrow(after(both[label, part], token) + wide(came[label, part]))
        far[label, part] = along_line(token, inner, forward)

    inward_step(FAR_END, 0)
    inward_step(FAR_MID, 0)
    token = narrow(after(have["other", OWN, 0], token) + wide(from_mate0[half:]))
    y[OWN, 0] = beside(token)
    inward_step(FAR_END, 1)
    forward_step(FAR_END, 0)
    inward_step(FAR_MID, 1)
    forward_step(FAR_MID, 0)
    token = narrow(after(have["keep", MATE, 1], token) + wide(y[MATE, 1]))
    from_mate1 = along_line(token, inner, mates)
    forward_step(FAR_END, 1)
    forward_step(FAR_MID, 1)
    own0 = after(have["keep", OWN, 0], token) + wide(from_mate0[:half]) + wide(y[OWN, 0])
    own1 = after(have["keep", OWN, 1], token) + wide(from_mate1) + wide(y[OWN, 1])
    return [
        own + wide(far[FAR_END, part]) + wide(far[FAR_MID, part]) for part, own in enumerate((own0, own1))
    ]


def scatter_sum_any(shot_data, code, owned):
    n_shot = lax.axis_size("shot")
    shot_dev, rcv_dev, samples = shot_data.shape
    me = lax.axis_index("shot")
    relative = [0]
    mask = 1
    while mask < n_shot:
        relative = relative + [e ^ mask for e in relative]
        mask *= 2
    wanted = me ^ jnp.array(relative, jnp.int32)
    signs = narrow(code).reshape(n_shot, owned, shot_dev)[wanted]
    total = jnp.einsum("eos,srt->eort", signs, shot_data, preferred_element_type=jnp.float32)
    while total.shape[0] > 1:
        count = total.shape[0] // 2
        total = total[:count] + wide(swap(narrow(total[count:]), "shot", n_shot, count))
    half = max(owned // 2, 1)
    return [total[0, low : low + half] for low in range(0, owned, half)]


def on_device(shot_data, code, observed, block_of, stencil_index, stencil_weight):
    shot_dev, rcv_dev, samples = shot_data.shape
    owned = observed.shape[0]
    if lax.axis_size("shot") == 2 * LINE and owned % 2 == 0:
        sums = scatter_sum_line(shot_data, code, owned)
    else:
        sums = scatter_sum_any(shot_data, code, owned)
    n_blocks = lax.axis_size("rcv")
    my_block = lax.axis_index("rcv")
    block_ids = block_of[:, 0]
    spread = spread_weights(stencil_index, stencil_weight)
    own_matrix = jnp.where(block_ids[None, :] == my_block, spread, 0.0).astype(jnp.bfloat16)
    ids = block_ids.reshape(n_blocks, rcv_dev)
    earlier = jnp.arange(rcv_dev)[None, None, :] < jnp.arange(rcv_dev)[None, :, None]
    rank = jnp.sum(jnp.where((ids[:, :, None] == ids[:, None, :]) & earlier, 1, 0), axis=2)
    my_ids = lax.dynamic_index_in_dim(ids, my_block, 0, keepdims=False)
    slot_rank = lax.dynamic_index_in_dim(rank, my_block, 0, keepdims=False)
    block_range = my_block ^ jnp.arange(n_blocks, dtype=jnp.int32)
    slot_range = jnp.arange(CAP, dtype=jnp.int32)
    selection = (my_ids[None, None, :] == block_range[:, None, None]) & (
        slot_rank[None, None, :] == slot_range[None, :, None]
    )
    selection = selection.reshape(n_blocks * CAP, rcv_dev).astype(jnp.bfloat16)
    pick_all = (
        (ids == my_block)[:, :, None] & (rank[:, :, None] == slot_range[None, None, :])
    ).astype(jnp.float32)
    slot_matrix = jnp.einsum(
        "gdr,drc->dgc", own_matrix.astype(jnp.float32).reshape(GRID, n_blocks, rcv_dev), pick_all
    ).astype(jnp.bfloat16)
    slot_matrix = jnp.stack(
        [lax.dynamic_index_in_dim(slot_matrix, my_block ^ e, 0, keepdims=False) for e in range(n_blocks)],
        axis=1,
    )
    slot_matrix = slot_matrix.reshape(GRID, n_blocks * CAP)
    results, at = [], 0
    for total in sums:
        residual = narrow(total - wide(observed[at : at + total.shape[0]]))
        at += total.shape[0]
        outgoing = narrow(jnp.einsum("sr,krt->kst", selection, residual, preferred_element_type=jnp.float32))
        pieces = [outgoing[:, :CAP]] + [
            swap(outgoing[:, e * CAP : (e + 1) * CAP], "rcv", n_blocks, e) for e in range(1, n_blocks)
        ]
        incoming = jnp.concatenate(pieces, axis=1)
        results.append(jnp.einsum("cs,kst->kct", slot_matrix, incoming, preferred_element_type=jnp.float32))
    return jnp.concatenate(results, axis=0)


def solution(mesh):
    placed = (P("shot", "rcv", None), P(None, "shot"), P("shot", "rcv", None), P(), P(), P())
    return jax.shard_map(
        on_device, mesh=mesh, in_specs=placed, out_specs=P("shot", "rcv", None), check_vma=False
    )
```

```python
import functools
import jax
import jax.numpy as jnp
from jax import lax
from jax.experimental import pallas as pl
from jax.experimental.pallas import tpu as pltpu
from jax.sharding import PartitionSpec as P

GRID = 256
CAP = 64
GROUP = 8
FAR_END, FAR_MID, MATE, OWN = range(4)
LINE = 4
SPARE_BYTES = 4 << 20
SMALL_BYTES = 12 << 20


def wide(value):
    return value.astype(jnp.float32)


def narrow(value):
    return value.astype(jnp.bfloat16)


def after(value, *earlier):
    return lax.optimization_barrier((value, *earlier))[0]


def swap(value, axis, size, mask):
    return lax.ppermute(value, axis, [(i, i ^ mask) for i in range(size)])


def along_line(value, inner, moves):
    pairs = [(a * inner + i, b * inner + i) for a, b in moves for i in range(inner)]
    return lax.ppermute(value, "shot", pairs)


def partial_sums_kernel(inner, owned, outputs, chunks, data_ref, code_ref, *refs):
    out_refs = refs[: len(outputs)]
    data, signs_ref, code_sem, data_sem = refs[len(outputs) :]
    shot_dev, rows, samples = data.shape
    block = rows // chunks
    code_copy = pltpu.make_async_copy(code_ref, signs_ref, code_sem)
    code_copy.start()
    copies = []
    for chunk in range(chunks):
        at = pl.ds(chunk * block, block)
        copies.append(pltpu.make_async_copy(data_ref.at[:, at, :], data.at[:, at, :], data_sem.at[chunk]))
        copies[-1].start()
    me = lax.axis_index("shot")
    place = lax.div(me, inner)
    column = lax.rem(me, inner)
    low = place < LINE // 2
    targets = {
        FAR_END: jnp.where(low, LINE - 1, 0),
        FAR_MID: jnp.where(low, LINE // 2, LINE // 2 - 1),
        MATE: place ^ 1,
        OWN: place,
    }
    width = shot_dev * GROUP
    shot = lax.broadcasted_iota(jnp.int32, (shot_dev, width), 0)
    lane = lax.broadcasted_iota(jnp.int32, (shot_dev, width), 1)
    spread = narrow(wide(shot == lane // GROUP))
    code_copy.wait()
    picked = []
    for wanted, _ in outputs:
        for label, other, row in wanted:
            at = (targets[label] * inner + (column ^ other)) * owned + row
            picked.append(jnp.broadcast_to(signs_ref[pl.ds(at, 1), :], (GROUP, shot_dev)))
    signs = narrow(jnp.concatenate(picked, axis=0).astype(jnp.float32))
    mixed = jnp.dot(signs, spread, preferred_element_type=jnp.float32)
    sub = lax.broadcasted_iota(jnp.int32, mixed.shape, 0)
    lane = lax.broadcasted_iota(jnp.int32, mixed.shape, 1)
    mix = narrow(jnp.where(sub % GROUP == lane % GROUP, mixed, 0.0))
    for chunk in range(chunks):
        copies[chunk].wait()
        for low_row in range(chunk * block, (chunk + 1) * block, GROUP):
            part = data[:, low_row : low_row + GROUP, :].reshape(width, samples)
            product = jnp.dot(mix, part, preferred_element_type=jnp.float32)
            at = 0
            for (wanted, _), ref in zip(outputs, out_refs):
                for entry in range(len(wanted)):
                    piece = product[at * GROUP : (at + 1) * GROUP]
                    ref[entry, low_row : low_row + GROUP, :] = piece.astype(ref.dtype)
                    at += 1


def partial_sums(shot_data, code, inner, owned, needs, name):
    names, outputs = list(needs), list(needs.values())
    shot_dev, rcv_dev, samples = shot_data.shape
    chunks = 4
    total = sum(len(w) for w, _ in outputs)
    shapes = [((len(w), rcv_dev, samples), t) for w, t in outputs]
    anywhere = pl.BlockSpec(memory_space=pltpu.HBM)
    held = sum(len(w) * jnp.dtype(t).itemsize for w, t in outputs) * rcv_dev * samples
    limit = held + shot_data.size * shot_data.dtype.itemsize + SPARE_BYTES
    results = pl.pallas_call(
        functools.partial(partial_sums_kernel, inner, owned, outputs, chunks),
        in_specs=[anywhere, anywhere],
        out_specs=[pl.BlockSpec(memory_space=pltpu.VMEM)] * len(outputs),
        out_shape=[pltpu.VMEM(s, t) for s, t in shapes],
        scratch_shapes=[
            pltpu.VMEM(shot_data.shape, shot_data.dtype),
            pltpu.VMEM(code.shape, code.dtype),
            pltpu.SemaphoreType.DMA,
            pltpu.SemaphoreType.DMA((chunks,)),
        ],
        cost_estimate=pl.CostEstimate(
            flops=2 * total * shot_dev * rcv_dev * samples * GROUP,
            bytes_accessed=2 * shot_data.size,
            transcendentals=0,
        ),
        compiler_params=pltpu.CompilerParams(vmem_limit_bytes=limit),
        name=name,
    )(pltpu.with_memory_space_constraint(shot_data, pltpu.HBM), pltpu.with_memory_space_constraint(code, pltpu.HBM))
    return dict(zip(names, results))


def scatter_sum_line(shot_data, code, owned):
    n_shot = lax.axis_size("shot")
    inner = n_shot // LINE
    half = owned // 2
    rows = [range(half), range(half, owned)]
    first, last = 0, LINE - 1
    mid, next_mid = LINE // 2 - 1, LINE // 2
    names, outputs = [], []

    def need(name, blocks, part, dtype):
        names.append(name)
        outputs.append(([(label, other, row) for label, other in blocks for row in rows[part]], dtype))

    need("mate0", [(MATE, 0), (MATE, 1)], 0, jnp.bfloat16)
    for part in (0, 1):
        for label in (FAR_END, FAR_MID):
            need(("send", label, part), [(label, 1)], part, jnp.bfloat16)
            need(("keep", label, part), [(label, 0)], part, jnp.float32)
    need(("send", MATE, 1), [(MATE, 1)], 1, jnp.bfloat16)
    need(("keep", MATE, 1), [(MATE, 0)], 1, jnp.float32)
    need(("keep", OWN, 0), [(OWN, 0)], 0, jnp.float32)
    need(("other", OWN, 0), [(OWN, 1)], 0, jnp.float32)
    need(("keep", OWN, 1), [(OWN, 0)], 1, jnp.float32)
    need(("send", OWN, 1), [(OWN, 1)], 1, jnp.bfloat16)
    have = partial_sums(shot_data, code, inner, owned, dict(zip(names, outputs)), "partial_sums")

    mates = [(first, mid), (mid, first), (last, next_mid), (next_mid, last)]
    inward = [(first, mid), (last, next_mid)]
    to_end = [(mid, last), (next_mid, first)]
    to_mid = [(mid, next_mid), (next_mid, mid)]

    def beside(value):
        return swap(value, "shot", n_shot, 1)

    y = {}
    y[FAR_END, 0] = beside(have["send", FAR_END, 0])
    from_mate0 = along_line(have["mate0"], inner, mates)
    y[FAR_MID, 0] = beside(have["send", FAR_MID, 0])
    y[FAR_END, 1] = beside(have["send", FAR_END, 1])
    y[FAR_MID, 1] = beside(have["send", FAR_MID, 1])
    y[MATE, 1] = beside(have["send", MATE, 1])
    y[OWN, 1] = beside(have["send", OWN, 1])
    both, came, far = {}, {}, {}
    token = have["mate0"]

    def inward_step(label, part):
        nonlocal token
        both[label, part] = after(have["keep", label, part], token) + wide(y[label, part])
        token = narrow(both[label, part])
        came[label, part] = along_line(token, inner, inward)

    def forward_step(label, part):
        nonlocal token
        forward = to_end if label == FAR_END else to_mid
        token = narrow(after(both[label, part], token) + wide(came[label, part]))
        far[label, part] = along_line(token, inner, forward)

    inward_step(FAR_END, 0)
    inward_step(FAR_MID, 0)
    token = narrow(after(have["other", OWN, 0], token) + wide(from_mate0[half:]))
    y[OWN, 0] = beside(token)
    inward_step(FAR_END, 1)
    forward_step(FAR_END, 0)
    inward_step(FAR_MID, 1)
    forward_step(FAR_MID, 0)
    token = narrow(after(have["keep", MATE, 1], token) + wide(y[MATE, 1]))
    from_mate1 = along_line(token, inner, mates)
    forward_step(FAR_END, 1)
    forward_step(FAR_MID, 1)
    own0 = after(have["keep", OWN, 0], token) + wide(from_mate0[:half]) + wide(y[OWN, 0])
    own1 = after(have["keep", OWN, 1], token) + wide(from_mate1) + wide(y[OWN, 1])
    return [
        own + wide(far[FAR_END, part]) + wide(far[FAR_MID, part]) for part, own in enumerate((own0, own1))
    ]


def scatter_sum_any(shot_data, code, owned):
    n_shot = lax.axis_size("shot")
    shot_dev, rcv_dev, samples = shot_data.shape
    me = lax.axis_index("shot")
    relative = [0]
    mask = 1
    while mask < n_shot:
        relative = relative + [e ^ mask for e in relative]
        mask *= 2
    wanted = me ^ jnp.array(relative, jnp.int32)
    signs = narrow(code).reshape(n_shot, owned, shot_dev)[wanted]
    total = jnp.einsum("eos,srt->eort", signs, shot_data, preferred_element_type=jnp.float32)
    while total.shape[0] > 1:
        count = total.shape[0] // 2
        total = total[:count] + wide(swap(narrow(total[count:]), "shot", n_shot, count))
    half = max(owned // 2, 1)
    return [total[0, low : low + half] for low in range(0, owned, half)]


def tables_kernel(n_blocks, cap, block_ref, index_ref, weight_ref, select_ref, slot_ref):
    me = lax.axis_index("rcv")
    rcv_dev = select_ref.shape[1]
    grid, stencil = slot_ref.shape[0], index_ref.shape[0]
    above = lax.broadcasted_iota(jnp.int32, (rcv_dev, rcv_dev), 0)
    along = lax.broadcasted_iota(jnp.int32, (rcv_dev, rcv_dev), 1)
    before = narrow(wide(above < along))
    names = lax.broadcasted_iota(jnp.int32, (n_blocks, rcv_dev), 0)
    points = lax.broadcasted_iota(jnp.int32, (grid, rcv_dev), 0)

    def ids_and_ranks(device):
        at = pl.ds(pl.multiple_of(device * rcv_dev, rcv_dev), rcv_dev)
        ids = block_ref[:, at]
        named = wide(ids == names)
        counts = jnp.dot(narrow(named), before, preferred_element_type=jnp.float32)
        return at, ids, jnp.sum(named * counts, axis=0, keepdims=True).astype(jnp.int32)

    _, ids, rank = ids_and_ranks(me)
    row = lax.broadcasted_iota(jnp.int32, select_ref.shape, 0)
    select_ref[...] = narrow(wide(((me ^ (row // cap)) == ids) & (row % cap == rank)))
    place = lax.broadcasted_iota(jnp.int32, (cap, rcv_dev), 0)
    columns = []
    for e in range(n_blocks):
        at, ids, rank = ids_and_ranks(me ^ e)
        spread = jnp.zeros((grid, rcv_dev), jnp.float32)
        for which in range(stencil):
            index = index_ref[which : which + 1, at]
            weight = weight_ref[which : which + 1, at]
            spread = spread + jnp.where(points == index, weight, 0.0)
        pick = narrow(wide((ids == me) & (place == rank)))
        columns.append(
            lax.dot_general(
                narrow(spread), pick, (((1,), (1,)), ((), ())), preferred_element_type=jnp.float32
            )
        )
    slot_ref[...] = narrow(jnp.concatenate(columns, axis=1))


def tables(block_of, stencil_index, stencil_weight, n_blocks, rcv_dev):
    slots = n_blocks * CAP
    whole = pl.BlockSpec(memory_space=pltpu.VMEM)
    return pl.pallas_call(
        functools.partial(tables_kernel, n_blocks, CAP),
        in_specs=[whole] * 3,
        out_specs=[whole] * 2,
        out_shape=[pltpu.VMEM((slots, rcv_dev), jnp.bfloat16), pltpu.VMEM((GRID, slots), jnp.bfloat16)],
        compiler_params=pltpu.CompilerParams(vmem_limit_bytes=SMALL_BYTES),
        cost_estimate=pl.CostEstimate(
            flops=2 * GRID * slots * rcv_dev, bytes_accessed=4 * slots * rcv_dev, transcendentals=0
        ),
        name="tables",
    )(block_of.T, stencil_index.T, stencil_weight.T)


def inject_kernel(halves, slot_ref, *refs):
    pieces, out_ref, built, sems = refs[:-3], refs[-3], refs[-2], refs[-1]
    per_half = len(pieces) // halves
    slots = slot_ref[...]
    copies, at = [], 0
    for part in range(halves):
        mine = pieces[part * per_half : (part + 1) * per_half]
        for row in range(mine[0].shape[0]):
            value = jnp.concatenate([ref[row] for ref in mine], axis=0)
            built[at] = jnp.dot(slots, value, preferred_element_type=jnp.float32)
            copies.append(pltpu.make_async_copy(built.at[at], out_ref.at[at], sems.at[at]))
            copies[-1].start()
            at += 1
    for copy in copies:
        copy.wait()


def inject(slot_matrix, groups):
    pieces = [piece for group in groups for piece in group]
    rows = sum(group[0].shape[0] for group in groups)
    shape = (rows, slot_matrix.shape[0], pieces[0].shape[2])
    whole = pl.BlockSpec(memory_space=pltpu.VMEM)
    return pl.pallas_call(
        functools.partial(inject_kernel, len(groups)),
        in_specs=[whole] * (1 + len(pieces)),
        out_specs=pl.BlockSpec(memory_space=pltpu.HBM),
        out_shape=jax.ShapeDtypeStruct(shape, jnp.float32),
        scratch_shapes=[pltpu.VMEM(shape, jnp.float32), pltpu.SemaphoreType.DMA((rows,))],
        compiler_params=pltpu.CompilerParams(vmem_limit_bytes=SMALL_BYTES),
        cost_estimate=pl.CostEstimate(
            flops=2 * rows * shape[1] * shape[2] * slot_matrix.shape[1],
            bytes_accessed=4 * rows * shape[1] * shape[2],
            transcendentals=0,
        ),
        name="inject",
    )(slot_matrix, *pieces)


def on_device(shot_data, code, observed, block_of, stencil_index, stencil_weight):
    shot_dev, rcv_dev, samples = shot_data.shape
    owned = observed.shape[0]
    if lax.axis_size("shot") == 2 * LINE and owned % 2 == 0:
        sums = scatter_sum_line(shot_data, code, owned)
    else:
        sums = scatter_sum_any(shot_data, code, owned)
    n_blocks = lax.axis_size("rcv")
    selection, slot_matrix = tables(block_of, stencil_index, stencil_weight, n_blocks, rcv_dev)
    groups, at = [], 0
    for total in sums:
        residual = narrow(total - wide(observed[at : at + total.shape[0]]))
        at += total.shape[0]
        outgoing = narrow(jnp.einsum("sr,krt->kst", selection, residual, preferred_element_type=jnp.float32))
        groups.append(
            [outgoing[:, :CAP]]
            + [swap(outgoing[:, e * CAP : (e + 1) * CAP], "rcv", n_blocks, e) for e in range(1, n_blocks)]
        )
    return inject(slot_matrix, groups)


def solution(mesh):
    placed = (P("shot", "rcv", None), P(None, "shot"), P("shot", "rcv", None), P(), P(), P())
    return jax.shard_map(
        on_device, mesh=mesh, in_specs=placed, out_specs=P("shot", "rcv", None), check_vma=False
    )
```

```python
import functools
import jax
import jax.numpy as jnp
from jax import lax
from jax.experimental import pallas as pl
from jax.experimental.pallas import tpu as pltpu
from jax.sharding import PartitionSpec as P

GRID = 256
CAP = 64
GROUP = 8
FAR_END, FAR_MID, MATE, OWN = range(4)
LINE = 4
SPARE_BYTES = 4 << 20
SMALL_BYTES = 12 << 20


def wide(value):
    return value.astype(jnp.float32)


def narrow(value):
    return value.astype(jnp.bfloat16)


def after(value, *earlier):
    return lax.optimization_barrier((value, *earlier))[0]


def swap(value, axis, size, mask):
    return lax.ppermute(value, axis, [(i, i ^ mask) for i in range(size)])


def along_line(value, inner, moves):
    pairs = [(a * inner + i, b * inner + i) for a, b in moves for i in range(inner)]
    return lax.ppermute(value, "shot", pairs)


def partial_sums_kernel(inner, owned, outputs, chunks, data_ref, code_ref, *refs):
    out_refs = refs[: len(outputs)]
    if chunks:
        data, signs_ref, code_sem, data_sem = refs[len(outputs) :]
    else:
        data, (signs_ref, code_sem) = data_ref, refs[len(outputs) :]
    shot_dev, rows, samples = data.shape
    block = rows // max(chunks, 1)
    code_copy = pltpu.make_async_copy(code_ref, signs_ref, code_sem)
    code_copy.start()
    copies = []
    for chunk in range(chunks):
        at = pl.ds(chunk * block, block)
        copies.append(pltpu.make_async_copy(data_ref.at[:, at, :], data.at[:, at, :], data_sem.at[chunk]))
        copies[-1].start()
    me = lax.axis_index("shot")
    place = lax.div(me, inner)
    column = lax.rem(me, inner)
    low = place < LINE // 2
    targets = {
        FAR_END: jnp.where(low, LINE - 1, 0),
        FAR_MID: jnp.where(low, LINE // 2, LINE // 2 - 1),
        MATE: place ^ 1,
        OWN: place,
    }
    width = shot_dev * GROUP
    shot = lax.broadcasted_iota(jnp.int32, (shot_dev, width), 0)
    lane = lax.broadcasted_iota(jnp.int32, (shot_dev, width), 1)
    spread = narrow(wide(shot == lane // GROUP))
    code_copy.wait()
    picked = []
    for wanted, _ in outputs:
        for label, other, row in wanted:
            at = (targets[label] * inner + (column ^ other)) * owned + row
            picked.append(jnp.broadcast_to(signs_ref[pl.ds(at, 1), :], (GROUP, shot_dev)))
    signs = narrow(jnp.concatenate(picked, axis=0).astype(jnp.float32))
    mixed = jnp.dot(signs, spread, preferred_element_type=jnp.float32)
    sub = lax.broadcasted_iota(jnp.int32, mixed.shape, 0)
    lane = lax.broadcasted_iota(jnp.int32, mixed.shape, 1)
    mix = narrow(jnp.where(sub % GROUP == lane % GROUP, mixed, 0.0))
    for chunk in range(max(chunks, 1)):
        if chunks:
            copies[chunk].wait()
        for low_row in range(chunk * block, (chunk + 1) * block, GROUP):
            part = data[:, low_row : low_row + GROUP, :].reshape(width, samples)
            product = jnp.dot(mix, part, preferred_element_type=jnp.float32)
            at = 0
            for (wanted, _), ref in zip(outputs, out_refs):
                for entry in range(len(wanted)):
                    piece = product[at * GROUP : (at + 1) * GROUP]
                    ref[entry, low_row : low_row + GROUP, :] = piece.astype(ref.dtype)
                    at += 1


def partial_sums(shot_data, code, inner, owned, needs, chunks, name):
    names, outputs = list(needs), list(needs.values())
    shot_dev, rcv_dev, samples = shot_data.shape
    total = sum(len(w) for w, _ in outputs)
    shapes = [((len(w), rcv_dev, samples), t) for w, t in outputs]
    scratch = [pltpu.VMEM(code.shape, code.dtype), pltpu.SemaphoreType.DMA]
    if chunks:
        shapes.append((shot_data.shape, shot_data.dtype))
        scratch.append(pltpu.SemaphoreType.DMA((chunks,)))
    space = pltpu.HBM if chunks else pltpu.VMEM
    held = sum(len(w) * jnp.dtype(t).itemsize for w, t in outputs) * rcv_dev * samples
    limit = held + shot_data.size * shot_data.dtype.itemsize + SPARE_BYTES
    results = pl.pallas_call(
        functools.partial(partial_sums_kernel, inner, owned, outputs, chunks),
        in_specs=[pl.BlockSpec(memory_space=space), pl.BlockSpec(memory_space=pltpu.HBM)],
        out_specs=[pl.BlockSpec(memory_space=pltpu.VMEM)] * len(shapes),
        out_shape=[pltpu.VMEM(s, t) for s, t in shapes],
        scratch_shapes=scratch,
        cost_estimate=pl.CostEstimate(
            flops=2 * total * shot_dev * rcv_dev * samples * GROUP,
            bytes_accessed=2 * shot_data.size,
            transcendentals=0,
        ),
        compiler_params=pltpu.CompilerParams(vmem_limit_bytes=limit),
        name=name,
    )(
        pltpu.with_memory_space_constraint(shot_data, space),
        pltpu.with_memory_space_constraint(code, pltpu.HBM),
    )
    return dict(zip(names, results)), results[-1]


def scatter_sum_line(shot_data, code, owned):
    n_shot = lax.axis_size("shot")
    inner = n_shot // LINE
    half = owned // 2
    rows = [range(half), range(half, owned)]
    first, last = 0, LINE - 1
    mid, next_mid = LINE // 2 - 1, LINE // 2
    names, outputs = [], []

    def need(name, blocks, part, dtype):
        names.append(name)
        outputs.append(([(label, other, row) for label, other in blocks for row in rows[part]], dtype))

    need("mate0", [(MATE, 0), (MATE, 1)], 0, jnp.bfloat16)
    for part in (0, 1):
        for label in (FAR_END, FAR_MID):
            need(("send", label, part), [(label, 1)], part, jnp.bfloat16)
            need(("keep", label, part), [(label, 0)], part, jnp.float32)
    need(("send", MATE, 1), [(MATE, 1)], 1, jnp.bfloat16)
    need(("keep", MATE, 1), [(MATE, 0)], 1, jnp.float32)
    need(("keep", OWN, 0), [(OWN, 0)], 0, jnp.float32)
    need(("other", OWN, 0), [(OWN, 1)], 0, jnp.float32)
    need(("keep", OWN, 1), [(OWN, 0)], 1, jnp.float32)
    need(("send", OWN, 1), [(OWN, 1)], 1, jnp.bfloat16)
    needs = dict(zip(names, outputs))
    leading = {name: needs.pop(name) for name in (("send", FAR_END, 0), "mate0", ("send", FAR_MID, 0))}
    have, shot_data = partial_sums(shot_data, code, inner, owned, leading, 4, "leading_sums")
    have |= partial_sums(shot_data, code, inner, owned, needs, 0, "trailing_sums")[0]

    mates = [(first, mid), (mid, first), (last, next_mid), (next_mid, last)]
    inward = [(first, mid), (last, next_mid)]
    to_end = [(mid, last), (next_mid, first)]
    to_mid = [(mid, next_mid), (next_mid, mid)]

    def beside(value):
        return swap(value, "shot", n_shot, 1)

    y = {}
    y[FAR_END, 0] = beside(have["send", FAR_END, 0])
    from_mate0 = along_line(have["mate0"], inner, mates)
    y[FAR_MID, 0] = beside(have["send", FAR_MID, 0])
    y[FAR_END, 1] = beside(have["send", FAR_END, 1])
    y[FAR_MID, 1] = beside(have["send", FAR_MID, 1])
    both, came, far = {}, {}, {}
    token = have["mate0"]

    def inward_step(label, part):
        nonlocal token
        both[label, part] = after(have["keep", label, part], token) + wide(y[label, part])
        token = narrow(both[label, part])
        came[label, part] = along_line(token, inner, inward)

    def forward_step(label, part):
        nonlocal token
        forward = to_end if label == FAR_END else to_mid
        token = narrow(after(both[label, part], token) + wide(came[label, part]))
        far[label, part] = along_line(token, inner, forward)

    inward_step(FAR_END, 0)
    y[MATE, 1] = beside(after(have["send", MATE, 1], token))
    y[OWN, 1] = beside(after(have["send", OWN, 1], token))
    inward_step(FAR_MID, 0)
    token = narrow(after(have["other", OWN, 0], token) + wide(from_mate0[half:]))
    y[OWN, 0] = beside(token)
    middle = token
    forward_step(FAR_END, 0)
    inward_step(FAR_END, 1)
    inward_step(FAR_MID, 1)
    forward_step(FAR_MID, 0)
    token = narrow(after(have["keep", MATE, 1], token) + wide(y[MATE, 1]))
    from_mate1 = along_line(token, inner, mates)
    forward_step(FAR_END, 1)
    forward_step(FAR_MID, 1)
    own0 = after(have["keep", OWN, 0], token) + wide(from_mate0[:half]) + wide(y[OWN, 0])
    own1 = after(have["keep", OWN, 1], token) + wide(from_mate1) + wide(y[OWN, 1])
    sums = [own + wide(far[FAR_END, part]) + wide(far[FAR_MID, part]) for part, own in enumerate((own0, own1))]
    return sums, middle


def scatter_sum_any(shot_data, code, owned):
    n_shot = lax.axis_size("shot")
    shot_dev, rcv_dev, samples = shot_data.shape
    me = lax.axis_index("shot")
    relative = [0]
    mask = 1
    while mask < n_shot:
        relative = relative + [e ^ mask for e in relative]
        mask *= 2
    wanted = me ^ jnp.array(relative, jnp.int32)
    signs = narrow(code).reshape(n_shot, owned, shot_dev)[wanted]
    total = jnp.einsum("eos,srt->eort", signs, shot_data, preferred_element_type=jnp.float32)
    while total.shape[0] > 1:
        count = total.shape[0] // 2
        total = total[:count] + wide(swap(narrow(total[count:]), "shot", n_shot, count))
    half = max(owned // 2, 1)
    return [total[0, low : low + half] for low in range(0, owned, half)]


def tables_kernel(n_blocks, cap, block_ref, index_ref, weight_ref, select_ref, slot_ref):
    me = lax.axis_index("rcv")
    rcv_dev = select_ref.shape[1]
    grid, stencil = slot_ref.shape[0], index_ref.shape[0]
    above = lax.broadcasted_iota(jnp.int32, (rcv_dev, rcv_dev), 0)
    along = lax.broadcasted_iota(jnp.int32, (rcv_dev, rcv_dev), 1)
    before = narrow(wide(above < along))
    names = lax.broadcasted_iota(jnp.int32, (n_blocks, rcv_dev), 0)
    points = lax.broadcasted_iota(jnp.int32, (grid, rcv_dev), 0)

    def ids_and_ranks(device):
        at = pl.ds(pl.multiple_of(device * rcv_dev, rcv_dev), rcv_dev)
        ids = block_ref[:, at]
        named = wide(ids == names)
        counts = jnp.dot(narrow(named), before, preferred_element_type=jnp.float32)
        return at, ids, jnp.sum(named * counts, axis=0, keepdims=True).astype(jnp.int32)

    _, ids, rank = ids_and_ranks(me)
    row = lax.broadcasted_iota(jnp.int32, select_ref.shape, 0)
    select_ref[...] = narrow(wide(((me ^ (row // cap)) == ids) & (row % cap == rank)))
    place = lax.broadcasted_iota(jnp.int32, (cap, rcv_dev), 0)
    columns = []
    for e in range(n_blocks):
        at, ids, rank = ids_and_ranks(me ^ e)
        spread = jnp.zeros((grid, rcv_dev), jnp.float32)
        for which in range(stencil):
            index = index_ref[which : which + 1, at]
            weight = weight_ref[which : which + 1, at]
            spread = spread + jnp.where(points == index, weight, 0.0)
        pick = narrow(wide((ids == me) & (place == rank)))
        columns.append(
            lax.dot_general(
                narrow(spread), pick, (((1,), (1,)), ((), ())), preferred_element_type=jnp.float32
            )
        )
    slot_ref[...] = narrow(jnp.concatenate(columns, axis=1))


def tables(block_of, stencil_index, stencil_weight, n_blocks, rcv_dev):
    slots = n_blocks * CAP
    whole = pl.BlockSpec(memory_space=pltpu.VMEM)
    return pl.pallas_call(
        functools.partial(tables_kernel, n_blocks, CAP),
        in_specs=[whole] * 3,
        out_specs=[whole] * 2,
        out_shape=[pltpu.VMEM((slots, rcv_dev), jnp.bfloat16), pltpu.VMEM((GRID, slots), jnp.bfloat16)],
        compiler_params=pltpu.CompilerParams(vmem_limit_bytes=SMALL_BYTES),
        cost_estimate=pl.CostEstimate(
            flops=2 * GRID * slots * rcv_dev, bytes_accessed=4 * slots * rcv_dev, transcendentals=0
        ),
        name="tables",
    )(block_of.T, stencil_index.T, stencil_weight.T)


def inject_kernel(first_row, slot_ref, *refs):
    pieces, out_ref, built, sems = refs[:-3], refs[-3], refs[-2], refs[-1]
    if first_row:
        pieces = pieces[:-1]
    slots = slot_ref[...]
    copies = []
    for row in range(pieces[0].shape[0]):
        value = jnp.concatenate([ref[row] for ref in pieces], axis=0)
        built[row] = jnp.dot(slots, value, preferred_element_type=jnp.float32)
        copies.append(pltpu.make_async_copy(built.at[row], out_ref.at[first_row + row], sems.at[row]))
        copies[-1].start()
    for copy in copies:
        copy.wait()


def inject(slot_matrix, pieces, rows, first_row, so_far):
    count, _, samples = pieces[0].shape
    grid, slots = slot_matrix.shape
    whole = pl.BlockSpec(memory_space=pltpu.VMEM)
    there = pl.BlockSpec(memory_space=pltpu.HBM)
    earlier = [] if so_far is None else [so_far]
    return pl.pallas_call(
        functools.partial(inject_kernel, first_row),
        in_specs=[whole] * (1 + len(pieces)) + [there] * len(earlier),
        out_specs=there,
        out_shape=jax.ShapeDtypeStruct((rows, grid, samples), jnp.float32),
        input_output_aliases={1 + len(pieces): 0} if earlier else {},
        scratch_shapes=[pltpu.VMEM((count, grid, samples), jnp.float32), pltpu.SemaphoreType.DMA((count,))],
        compiler_params=pltpu.CompilerParams(vmem_limit_bytes=SMALL_BYTES),
        cost_estimate=pl.CostEstimate(
            flops=2 * count * grid * samples * slots, bytes_accessed=4 * count * grid * samples, transcendentals=0
        ),
        name="inject",
    )(slot_matrix, *pieces, *earlier)


def on_device(shot_data, code, observed, block_of, stencil_index, stencil_weight):
    shot_dev, rcv_dev, samples = shot_data.shape
    owned = observed.shape[0]
    if lax.axis_size("shot") == 2 * LINE and owned % 2 == 0:
        sums, middle = scatter_sum_line(shot_data, code, owned)
        block_of, stencil_index, stencil_weight, _ = lax.optimization_barrier(
            (block_of, stencil_index, stencil_weight, middle)
        )
    else:
        sums = scatter_sum_any(shot_data, code, owned)
    n_blocks = lax.axis_size("rcv")
    selection, slot_matrix = tables(block_of, stencil_index, stencil_weight, n_blocks, rcv_dev)
    result, outgoing, at = None, None, 0
    for total in sums:
        seen = observed[at : at + total.shape[0]]
        if outgoing is not None:
            seen = after(seen, outgoing)
        residual = narrow(total - wide(seen))
        outgoing = narrow(jnp.einsum("sr,krt->kst", selection, residual, preferred_element_type=jnp.float32))
        pieces = [outgoing[:, :CAP]] + [
            swap(outgoing[:, e * CAP : (e + 1) * CAP], "rcv", n_blocks, e) for e in range(1, n_blocks)
        ]
        result = inject(slot_matrix, pieces, owned, at, result)
        at += total.shape[0]
    return result


def solution(mesh):
    placed = (P("shot", "rcv", None), P(None, "shot"), P("shot", "rcv", None), P(), P(), P())
    return jax.shard_map(
        on_device, mesh=mesh, in_specs=placed, out_specs=P("shot", "rcv", None), check_vma=False
    )
```

```python
import functools
import jax
import jax.numpy as jnp
from jax import lax
from jax.experimental import pallas as pl
from jax.experimental.pallas import tpu as pltpu
from jax.sharding import PartitionSpec as P

GRID = 256
CAP = 64
GROUP = 8
FAR_END, FAR_MID, MATE, OWN = range(4)
LINE = 4
SPARE_BYTES = 4 << 20
SMALL_BYTES = 12 << 20


def wide(value):
    return value.astype(jnp.float32)


def narrow(value):
    return value.astype(jnp.bfloat16)


def after(value, *earlier):
    return lax.optimization_barrier((value, *earlier))[0]


def swap(value, axis, size, mask):
    return lax.ppermute(value, axis, [(i, i ^ mask) for i in range(size)])


def along_line(value, inner, moves):
    pairs = [(a * inner + i, b * inner + i) for a, b in moves for i in range(inner)]
    return lax.ppermute(value, "shot", pairs)


def partial_sums_kernel(inner, owned, outputs, chunks, data_ref, code_ref, *refs):
    out_refs = refs[: len(outputs)]
    if chunks:
        data, signs_ref, code_sem, data_sem = refs[len(outputs) :]
    else:
        data, (signs_ref, code_sem) = data_ref, refs[len(outputs) :]
    shot_dev, rows, samples = data.shape
    block = rows // max(chunks, 1)
    code_copy = pltpu.make_async_copy(code_ref, signs_ref, code_sem)
    code_copy.start()
    copies = []
    for chunk in range(chunks):
        at = pl.ds(chunk * block, block)
        copies.append(pltpu.make_async_copy(data_ref.at[:, at, :], data.at[:, at, :], data_sem.at[chunk]))
        copies[-1].start()
    me = lax.axis_index("shot")
    place = lax.div(me, inner)
    column = lax.rem(me, inner)
    low = place < LINE // 2
    targets = {
        FAR_END: jnp.where(low, LINE - 1, 0),
        FAR_MID: jnp.where(low, LINE // 2, LINE // 2 - 1),
        MATE: place ^ 1,
        OWN: place,
    }
    width = shot_dev * GROUP
    shot = lax.broadcasted_iota(jnp.int32, (shot_dev, width), 0)
    lane = lax.broadcasted_iota(jnp.int32, (shot_dev, width), 1)
    spread = narrow(wide(shot == lane // GROUP))
    code_copy.wait()
    picked = []
    for wanted, _ in outputs:
        for label, other, row in wanted:
            at = (targets[label] * inner + (column ^ other)) * owned + row
            picked.append(jnp.broadcast_to(signs_ref[pl.ds(at, 1), :], (GROUP, shot_dev)))
    signs = narrow(jnp.concatenate(picked, axis=0).astype(jnp.float32))
    mixed = jnp.dot(signs, spread, preferred_element_type=jnp.float32)
    sub = lax.broadcasted_iota(jnp.int32, mixed.shape, 0)
    lane = lax.broadcasted_iota(jnp.int32, mixed.shape, 1)
    mix = narrow(jnp.where(sub % GROUP == lane % GROUP, mixed, 0.0))
    for chunk in range(max(chunks, 1)):
        if chunks:
            copies[chunk].wait()
        for low_row in range(chunk * block, (chunk + 1) * block, GROUP):
            part = data[:, low_row : low_row + GROUP, :].reshape(width, samples)
            product = jnp.dot(mix, part, preferred_element_type=jnp.float32)
            at = 0
            for (wanted, _), ref in zip(outputs, out_refs):
                for entry in range(len(wanted)):
                    piece = product[at * GROUP : (at + 1) * GROUP]
                    ref[entry, low_row : low_row + GROUP, :] = piece.astype(ref.dtype)
                    at += 1


def partial_sums(shot_data, code, inner, owned, needs, chunks, name):
    names, outputs = list(needs), list(needs.values())
    shot_dev, rcv_dev, samples = shot_data.shape
    total = sum(len(w) for w, _ in outputs)
    shapes = [((len(w), rcv_dev, samples), t) for w, t in outputs]
    scratch = [pltpu.VMEM(code.shape, code.dtype), pltpu.SemaphoreType.DMA]
    if chunks:
        shapes.append((shot_data.shape, shot_data.dtype))
        scratch.append(pltpu.SemaphoreType.DMA((chunks,)))
    space = pltpu.HBM if chunks else pltpu.VMEM
    held = sum(len(w) * jnp.dtype(t).itemsize for w, t in outputs) * rcv_dev * samples
    limit = held + shot_data.size * shot_data.dtype.itemsize + SPARE_BYTES
    results = pl.pallas_call(
        functools.partial(partial_sums_kernel, inner, owned, outputs, chunks),
        in_specs=[pl.BlockSpec(memory_space=space), pl.BlockSpec(memory_space=pltpu.HBM)],
        out_specs=[pl.BlockSpec(memory_space=pltpu.VMEM)] * len(shapes),
        out_shape=[pltpu.VMEM(s, t) for s, t in shapes],
        scratch_shapes=scratch,
        cost_estimate=pl.CostEstimate(
            flops=2 * total * shot_dev * rcv_dev * samples * GROUP,
            bytes_accessed=2 * shot_data.size,
            transcendentals=0,
        ),
        compiler_params=pltpu.CompilerParams(vmem_limit_bytes=limit),
        name=name,
    )(
        pltpu.with_memory_space_constraint(shot_data, space),
        pltpu.with_memory_space_constraint(code, pltpu.HBM),
    )
    return dict(zip(names, results)), results[-1]


def scatter_sum_line(shot_data, code, owned):
    n_shot = lax.axis_size("shot")
    inner = n_shot // LINE
    half = owned // 2
    rows = [range(half), range(half, owned)]
    first, last = 0, LINE - 1
    mid, next_mid = LINE // 2 - 1, LINE // 2
    names, outputs = [], []

    def need(name, blocks, part, dtype):
        names.append(name)
        outputs.append(([(label, other, row) for label, other in blocks for row in rows[part]], dtype))

    need("mate0", [(MATE, 0), (MATE, 1)], 0, jnp.bfloat16)
    for part in (0, 1):
        for label in (FAR_END, FAR_MID):
            need(("send", label, part), [(label, 1)], part, jnp.bfloat16)
            need(("keep", label, part), [(label, 0)], part, jnp.float32)
    need(("send", MATE, 1), [(MATE, 1)], 1, jnp.bfloat16)
    need(("keep", MATE, 1), [(MATE, 0)], 1, jnp.float32)
    need(("keep", OWN, 0), [(OWN, 0)], 0, jnp.float32)
    need(("other", OWN, 0), [(OWN, 1)], 0, jnp.float32)
    need(("keep", OWN, 1), [(OWN, 0)], 1, jnp.float32)
    need(("send", OWN, 1), [(OWN, 1)], 1, jnp.bfloat16)
    needs = dict(zip(names, outputs))
    leading = {name: needs.pop(name) for name in (("send", FAR_END, 0), "mate0", ("send", FAR_MID, 0))}
    have, shot_data = partial_sums(shot_data, code, inner, owned, leading, 2, "leading_sums")
    have |= partial_sums(shot_data, code, inner, owned, needs, 0, "trailing_sums")[0]

    mates = [(first, mid), (mid, first), (last, next_mid), (next_mid, last)]
    inward = [(first, mid), (last, next_mid)]
    to_end = [(mid, last), (next_mid, first)]
    to_mid = [(mid, next_mid), (next_mid, mid)]

    def beside(value):
        return swap(value, "shot", n_shot, 1)

    y = {}
    y[FAR_END, 0] = beside(have["send", FAR_END, 0])
    from_mate0 = along_line(have["mate0"], inner, mates)
    y[FAR_MID, 0] = beside(have["send", FAR_MID, 0])
    y[FAR_END, 1] = beside(have["send", FAR_END, 1])
    y[FAR_MID, 1] = beside(have["send", FAR_MID, 1])
    both, came, far = {}, {}, {}
    token = have["mate0"]

    def inward_step(label, part):
        nonlocal token
        both[label, part] = after(have["keep", label, part], token) + wide(y[label, part])
        token = narrow(both[label, part])
        came[label, part] = along_line(token, inner, inward)

    def forward_step(label, part):
        nonlocal token
        forward = to_end if label == FAR_END else to_mid
        token = narrow(after(both[label, part], token) + wide(came[label, part]))
        far[label, part] = along_line(token, inner, forward)

    inward_step(FAR_END, 0)
    y[MATE, 1] = beside(after(have["send", MATE, 1], token))
    y[OWN, 1] = beside(after(have["send", OWN, 1], token))
    inward_step(FAR_MID, 0)
    token = narrow(after(have["other", OWN, 0], token) + wide(from_mate0[half:]))
    y[OWN, 0] = beside(token)
    middle = token
    forward_step(FAR_END, 0)
    inward_step(FAR_END, 1)
    inward_step(FAR_MID, 1)
    forward_step(FAR_MID, 0)
    token = narrow(after(have["keep", MATE, 1], token) + wide(y[MATE, 1]))
    from_mate1 = along_line(token, inner, mates)
    forward_step(FAR_END, 1)
    forward_step(FAR_MID, 1)
    own0 = after(have["keep", OWN, 0], token) + wide(from_mate0[:half]) + wide(y[OWN, 0])
    own1 = after(have["keep", OWN, 1], token) + wide(from_mate1) + wide(y[OWN, 1])
    sums = [own + wide(far[FAR_END, part]) + wide(far[FAR_MID, part]) for part, own in enumerate((own0, own1))]
    return sums, middle


def scatter_sum_any(shot_data, code, owned):
    n_shot = lax.axis_size("shot")
    shot_dev, rcv_dev, samples = shot_data.shape
    me = lax.axis_index("shot")
    relative = [0]
    mask = 1
    while mask < n_shot:
        relative = relative + [e ^ mask for e in relative]
        mask *= 2
    wanted = me ^ jnp.array(relative, jnp.int32)
    signs = narrow(code).reshape(n_shot, owned, shot_dev)[wanted]
    total = jnp.einsum("eos,srt->eort", signs, shot_data, preferred_element_type=jnp.float32)
    while total.shape[0] > 1:
        count = total.shape[0] // 2
        total = total[:count] + wide(swap(narrow(total[count:]), "shot", n_shot, count))
    half = max(owned // 2, 1)
    return [total[0, low : low + half] for low in range(0, owned, half)]


def tables_kernel(n_blocks, cap, block_ref, index_ref, weight_ref, select_ref, slot_ref):
    me = lax.axis_index("rcv")
    rcv_dev = select_ref.shape[1]
    grid, stencil = slot_ref.shape[0], index_ref.shape[0]
    above = lax.broadcasted_iota(jnp.int32, (rcv_dev, rcv_dev), 0)
    along = lax.broadcasted_iota(jnp.int32, (rcv_dev, rcv_dev), 1)
    before = narrow(wide(above < along))
    names = lax.broadcasted_iota(jnp.int32, (n_blocks, rcv_dev), 0)
    points = lax.broadcasted_iota(jnp.int32, (grid, rcv_dev), 0)

    def ids_and_ranks(device):
        at = pl.ds(pl.multiple_of(device * rcv_dev, rcv_dev), rcv_dev)
        ids = block_ref[:, at]
        named = wide(ids == names)
        counts = jnp.dot(narrow(named), before, preferred_element_type=jnp.float32)
        return at, ids, jnp.sum(named * counts, axis=0, keepdims=True).astype(jnp.int32)

    _, ids, rank = ids_and_ranks(me)
    row = lax.broadcasted_iota(jnp.int32, select_ref.shape, 0)
    select_ref[...] = narrow(wide(((me ^ (row // cap)) == ids) & (row % cap == rank)))
    place = lax.broadcasted_iota(jnp.int32, (cap, rcv_dev), 0)
    columns = []
    for e in range(n_blocks):
        at, ids, rank = ids_and_ranks(me ^ e)
        spread = jnp.zeros((grid, rcv_dev), jnp.float32)
        for which in range(stencil):
            index = index_ref[which : which + 1, at]
            weight = weight_ref[which : which + 1, at]
            spread = spread + jnp.where(points == index, weight, 0.0)
        pick = narrow(wide((ids == me) & (place == rank)))
        columns.append(
            lax.dot_general(
                narrow(spread), pick, (((1,), (1,)), ((), ())), preferred_element_type=jnp.float32
            )
        )
    slot_ref[...] = narrow(jnp.concatenate(columns, axis=1))


def tables(block_of, stencil_index, stencil_weight, n_blocks, rcv_dev):
    slots = n_blocks * CAP
    whole = pl.BlockSpec(memory_space=pltpu.VMEM)
    return pl.pallas_call(
        functools.partial(tables_kernel, n_blocks, CAP),
        in_specs=[whole] * 3,
        out_specs=[whole] * 2,
        out_shape=[pltpu.VMEM((slots, rcv_dev), jnp.bfloat16), pltpu.VMEM((GRID, slots), jnp.bfloat16)],
        compiler_params=pltpu.CompilerParams(vmem_limit_bytes=SMALL_BYTES),
        cost_estimate=pl.CostEstimate(
            flops=2 * GRID * slots * rcv_dev, bytes_accessed=4 * slots * rcv_dev, transcendentals=0
        ),
        name="tables",
    )(block_of.T, stencil_index.T, stencil_weight.T)


def inject_kernel(first_row, slot_ref, *refs):
    pieces, out_ref, built, sems = refs[:-3], refs[-3], refs[-2], refs[-1]
    if first_row:
        pieces = pieces[:-1]
    slots = slot_ref[...]
    copies = []
    for row in range(pieces[0].shape[0]):
        value = jnp.concatenate([ref[row] for ref in pieces], axis=0)
        built[row] = jnp.dot(slots, value, preferred_element_type=jnp.float32)
        copies.append(pltpu.make_async_copy(built.at[row], out_ref.at[first_row + row], sems.at[row]))
        copies[-1].start()
    for copy in copies:
        copy.wait()


def inject(slot_matrix, pieces, rows, first_row, so_far):
    count, _, samples = pieces[0].shape
    grid, slots = slot_matrix.shape
    whole = pl.BlockSpec(memory_space=pltpu.VMEM)
    there = pl.BlockSpec(memory_space=pltpu.HBM)
    earlier = [] if so_far is None else [so_far]
    return pl.pallas_call(
        functools.partial(inject_kernel, first_row),
        in_specs=[whole] * (1 + len(pieces)) + [there] * len(earlier),
        out_specs=there,
        out_shape=jax.ShapeDtypeStruct((rows, grid, samples), jnp.float32),
        input_output_aliases={1 + len(pieces): 0} if earlier else {},
        scratch_shapes=[pltpu.VMEM((count, grid, samples), jnp.float32), pltpu.SemaphoreType.DMA((count,))],
        compiler_params=pltpu.CompilerParams(vmem_limit_bytes=SMALL_BYTES),
        cost_estimate=pl.CostEstimate(
            flops=2 * count * grid * samples * slots, bytes_accessed=4 * count * grid * samples, transcendentals=0
        ),
        name="inject",
    )(slot_matrix, *pieces, *earlier)


def on_device(shot_data, code, observed, block_of, stencil_index, stencil_weight):
    shot_dev, rcv_dev, samples = shot_data.shape
    owned = observed.shape[0]
    if lax.axis_size("shot") == 2 * LINE and owned % 2 == 0:
        sums, middle = scatter_sum_line(shot_data, code, owned)
        block_of, stencil_index, stencil_weight, _ = lax.optimization_barrier(
            (block_of, stencil_index, stencil_weight, middle)
        )
    else:
        sums = scatter_sum_any(shot_data, code, owned)
    n_blocks = lax.axis_size("rcv")
    selection, slot_matrix = tables(block_of, stencil_index, stencil_weight, n_blocks, rcv_dev)
    result, outgoing, at = None, None, 0
    for total in sums:
        seen = observed[at : at + total.shape[0]]
        if outgoing is not None:
            seen = after(seen, outgoing)
        residual = narrow(total - wide(seen))
        outgoing = narrow(jnp.einsum("sr,krt->kst", selection, residual, preferred_element_type=jnp.float32))
        pieces = [outgoing[:, :CAP]] + [
            swap(outgoing[:, e * CAP : (e + 1) * CAP], "rcv", n_blocks, e) for e in range(1, n_blocks)
        ]
        result = inject(slot_matrix, pieces, owned, at, result)
        at += total.shape[0]
    return result


def solution(mesh):
    placed = (P("shot", "rcv", None), P(None, "shot"), P("shot", "rcv", None), P(), P(), P())
    return jax.shard_map(
        on_device, mesh=mesh, in_specs=placed, out_specs=P("shot", "rcv", None), check_vma=False
    )
```
